32 devices in a mesh: rows: 8 (over y, x, core), cols: 4 (over z).
Axes of the slice: x: 2, y: 2, z: 4, core: 2. Of those that a mesh axis runs over, the one named last changes fastest.
Arguments:
- coarse: float32 [512, 512], P('rows', 'cols'), may hold values from -6 to 6
- detail4: float32 [3, 512, 512], P(None, 'rows', 'cols'), may hold values from -6 to 6
- detail3: float32 [3, 1024, 1024], P(None, 'rows', 'cols'), may hold values from -6 to 6
- detail2: float32 [3, 2048, 2048], P(None, 'rows', 'cols'), may hold values from -6 to 6
- detail1: float32 [3, 4096, 4096], P(None, 'rows', 'cols'), may hold values from -6 to 6
Outputs:
- image: float32 [8192, 8192], P('rows', 'cols')
The draws below stay inside these ranges and needn't reach their ends.
All inputs are finite; a program needn't handle non-finite values.
Results may differ from the reference program's by a relative error of at most 0.00013.
Values sent between devices are 32-bit elements; how exact they have to be, the bound alone decides.
A program may use at most 128 MiB of HBM per device.

```python
import jax
import jax.numpy as jnp

NR = 8192
NC = 8192


def steps_of(rng, dims, shards, smallest, high):
    def one(position, blocks):
        draws = jax.random.uniform(jax.random.fold_in(jax.random.fold_in(rng, 6), position), (blocks,), jnp.float32, smallest / len(shards), high / len(shards))
        return jnp.repeat(jnp.exp(draws), dims[position] // blocks).reshape((-1,) + (1,) * (len(dims) - position - 1))

    loudness = one(*shards[0])
    for cut in shards[1:]:
        loudness = loudness * one(*cut)
    return loudness


def noise(own_key, extent, deviation, reach, cuts=(), kind=jnp.bfloat16):
    result = deviation * jax.random.normal(own_key, extent, jnp.float32)
    if cuts:
        result = result * steps_of(own_key, extent, cuts, -0.22, 0.18)
    return jnp.clip(result, -reach, reach).astype(kind)


def setup_inputs(seed: int = 0) -> dict:
    splits = jax.random.split(jax.random.key(seed), 6)
    coarse = noise(splits[0], (NR // 16, NC // 16), 1.0, 6.0, ((0, 8), (1, 4)), jnp.float32)
    detail4 = noise(splits[1], (3, NR // 16, NC // 16), 1.0, 6.0, ((1, 8), (2, 4)), jnp.float32)
    detail3 = noise(splits[2], (3, NR // 8, NC // 8), 1.0, 6.0, ((1, 8), (2, 4)), jnp.float32)
    detail2 = noise(splits[3], (3, NR // 4, NC // 4), 1.0, 6.0, ((1, 8), (2, 4)), jnp.float32)
    detail1 = noise(splits[4], (3, NR // 2, NC // 2), 1.0, 6.0, ((1, 8), (2, 4)), jnp.float32)
    return {"coarse": coarse, "detail4": detail4, "detail3": detail3, "detail2": detail2, "detail1": detail1}


lift_alpha = -1.586134342059924
lift_beta = -0.052980118572961
lift_gamma = 0.882911075530934
lift_delta = 0.443506852043971
lift_scale = 1.149604398860241


def phase_join(smooth, rough, along):
    target = list(smooth.shape)
    target[along] = 2 * target[along]
    return jnp.stack((smooth, rough), axis=along + 1).reshape(target)


def lift_roll(smooth, rough, along):
    smooth = smooth * lift_scale
    rough = rough / lift_scale
    smooth = smooth - lift_delta * (rough + jnp.roll(rough, 1, along))
    rough = rough - lift_gamma * (smooth + jnp.roll(smooth, -1, along))
    smooth = smooth - lift_beta * (rough + jnp.roll(rough, 1, along))
    rough = rough - lift_alpha * (smooth + jnp.roll(smooth, -1, along))
    return phase_join(smooth, rough, along)


def whole_synth(lowband, detail):
    smooth = jnp.stack((lowband, detail[1]), 0)
    rough = jnp.stack((detail[0], detail[2]), 0)
    halves = lift_roll(smooth, rough, 2)
    return lift_roll(halves[0], halves[1], 0)


def reference(coarse, detail4, detail3, detail2, detail1):
    lowband = coarse
    for detail in (detail4, detail3, detail2, detail1):
        lowband = whole_synth(lowband, detail)
    return lowband
```

```python
import functools

import jax
import jax.numpy as jnp
from jax import lax
from jax.experimental import pallas as pl
from jax.experimental.pallas import tpu as pltpu
from jax.sharding import PartitionSpec as P

lift_alpha = -1.586134342059924
lift_beta = -0.052980118572961
lift_gamma = 0.882911075530934
lift_delta = 0.443506852043971
lift_scale = 1.149604398860241

MESH = pl.DeviceIdType.MESH
LANES = 128
SUB = 8


def groups_of(height):
    return min(16, height // SUB)


def lanes_of(shape):
    return lax.broadcasted_iota(jnp.int32, shape, len(shape) - 1)


def rows_of(shape):
    return lax.broadcasted_iota(jnp.int32, shape, len(shape) - 2)


def exchange(mesh_shape, levels, *refs):
    count = len(levels)
    inputs, refs = refs[:count], refs[count:]
    below, above, refs = refs[:count], refs[count : 2 * count], refs[2 * count :]
    from_right, from_left, down_right, down_left, up_right, up_left, *refs = refs
    packed, top, bottom, *refs = refs
    firsts, lasts, refs = refs[:count], refs[count : 2 * count], refs[2 * count :]
    local_sem, send_sem, recv_sem = refs

    n_rows, n_cols = mesh_shape
    row, col = lax.axis_index("rows"), lax.axis_index("cols")
    row_next, row_prev = lax.rem(row + 1, n_rows), lax.rem(row + n_rows - 1, n_rows)
    col_next, col_prev = lax.rem(col + 1, n_cols), lax.rem(col + n_cols - 1, n_cols)

    barrier = pltpu.get_barrier_semaphore()
    neighbours = [
        (r, c)
        for r in (row_prev, row, row_next)
        for c in (col_prev, col, col_next)
        if not (r is row and c is col)
    ]
    for place in neighbours:
        pl.semaphore_signal(barrier, inc=1, device_id=place, device_id_type=MESH)

    loads = []
    for i, (bands, height, width) in enumerate(levels):
        for j, (slab, start) in enumerate(((firsts[i], 0), (lasts[i], width - LANES))):
            copy = pltpu.make_async_copy(
                inputs[i].at[:, :, pl.ds(start, LANES)], slab, local_sem.at[2 * i + j]
            )
            copy.start()
            loads.append(copy)

    pl.semaphore_wait(barrier, len(neighbours))

    sends = []

    def send(src, dst, place):
        k = len(sends)
        copy = pltpu.make_async_remote_copy(
            src_ref=src,
            dst_ref=dst,
            send_sem=send_sem.at[k],
            recv_sem=recv_sem.at[k],
            device_id=place,
            device_id_type=MESH,
        )
        copy.start()
        sends.append(copy)

    for i in reversed(range(count)):
        height = levels[i][1]
        send(inputs[i].at[:, pl.ds(0, SUB), :], below[i], (row_prev, col))
        send(inputs[i].at[:, pl.ds(height - SUB, SUB), :], above[i], (row_next, col))

    for copy in loads:
        copy.wait()

    tops = bottoms = None
    offset = place = 0
    for i, (bands, height, width) in enumerate(levels):
        groups = groups_of(height)
        part = height // groups
        lane = lanes_of((part, LANES))
        slot = lax.rem(lane + 4, LANES) // 8
        lane8 = lanes_of((SUB, LANES))
        slot8 = lax.rem(lane8 + 4, LANES) // 8
        for b in range(bands):
            total = None
            for g in range(groups):
                rows = pl.ds(g * part, part)
                edge = jnp.where(lane < 64, firsts[i][b, rows, :], lasts[i][b, rows, :])
                if g:
                    edge = pltpu.roll(edge, 8 * g, 1)
                total = edge if total is None else jnp.where(slot == g, edge, total)
            packed[pl.ds(offset, part), :] = total
            offset += part
            for end in range(2):
                rows = pl.ds(0 if end == 0 else height - SUB, SUB)
                edge = jnp.where(lane8 < 64, firsts[i][b, rows, :], lasts[i][b, rows, :])
                if place:
                    edge = pltpu.roll(edge, 8 * place, 1)
                if end == 0:
                    tops = edge if tops is None else jnp.where(slot8 == place, edge, tops)
                else:
                    bottoms = edge if bottoms is None else jnp.where(slot8 == place, edge, bottoms)
            place += 1
    top[...] = tops
    bottom[...] = bottoms

    send(packed, from_right, (row, col_prev))
    send(packed, from_left, (row, col_next))
    send(top, down_right, (row_prev, col_prev))
    send(top, down_left, (row_prev, col_next))
    send(bottom, up_right, (row_next, col_prev))
    send(bottom, up_left, (row_next, col_next))
    for copy in sends:
        copy.wait()


def lifted(smooth, rough, before, after):
    smooth = smooth - lift_delta * (rough + before(rough))
    rough = rough - lift_gamma * (smooth + after(smooth))
    smooth = smooth - lift_beta * (rough + before(rough))
    rough = rough - lift_alpha * (smooth + after(smooth))
    return smooth, rough


def synthesis(sizes, chunk_rows, *refs):
    count = len(sizes)
    arrays = count + 1
    inputs, refs = refs[:arrays], refs[arrays:]
    below, above, refs = refs[:arrays], refs[arrays : 2 * arrays], refs[2 * arrays :]
    from_right, from_left, down_right, down_left, up_right, up_left, out, *refs = refs
    bands, joined, refs = refs[:count], refs[count], refs[count + 1 :]
    finished, load_sem, store_sem = refs

    loads = []
    k = 0
    for level, (height, width) in enumerate(sizes):
        mine = []
        for c in range(width // LANES):
            columns = pl.ds(c * LANES, LANES)
            if level == 0:
                copy = pltpu.make_async_copy(
                    inputs[0].at[:, :, columns],
                    bands[0].at[pl.ds(0, 1), c, pl.ds(0, height), :],
                    load_sem.at[k],
                )
                copy.start()
                mine.append(copy)
                k += 1
            copy = pltpu.make_async_copy(
                inputs[level + 1].at[:, :, columns],
                bands[level].at[pl.ds(1, 3), c, pl.ds(0, height), :],
                load_sem.at[k],
            )
            copy.start()
            mine.append(copy)
            k += 1
        loads.append(mine)

    lane = lanes_of((SUB, LANES))
    sub = rows_of((SUB, LANES))
    even = lax.rem(lane, 2) == 0
    low = lane < 64
    pick_low = lane // 2 + jnp.where(even, 0, 64)
    pick_high = lane // 2 + jnp.where(even, 64, 0)
    right_side = lax.rem(lane, 8) < 4

    corner = jnp.where(
        sub < 4,
        jnp.where(right_side, down_right[...], down_left[...]),
        jnp.where(right_side, up_right[...], up_left[...]),
    )
    offset = place = 0
    for i in range(arrays):
        level = max(i - 1, 0)
        height, width = sizes[level]
        groups = groups_of(height)
        part = height // groups
        tiles = width // LANES
        wide = lax.rem(lanes_of((part, LANES)), 8) < 4
        for b in range(1 if i == 0 else 3):
            ref = bands[level].at[b if i == 0 else b + 1]
            rows = pl.ds(offset, part)
            edge = jnp.where(wide, from_right[rows, :], from_left[rows, :])
            for g in range(groups):
                ref[tiles, pl.ds(g * part, part), :] = (
                    pltpu.roll(edge, LANES - 8 * g, 1) if g else edge
                )
            offset += part
            for c in range(tiles):
                columns = pl.ds(c * LANES, LANES)
                ref[c, pl.ds(height, SUB), :] = jnp.where(
                    sub < 4, below[i][b, :, columns], above[i][b, :, columns]
                )
            ref[tiles, pl.ds(height, SUB), :] = (
                pltpu.roll(corner, LANES - 8 * place, 1) if place else corner
            )
            place += 1

    big, small = lift_scale * lift_scale, 1.0 / (lift_scale * lift_scale)

    def vertical(ref, c, start, length, before, after):
        def window(b):
            body = ref[b, c, pl.ds(start, length), :]
            halo = jnp.where(
                sub < 4, ref[b, c, pl.ds(after, SUB), :], ref[b, c, pl.ds(before, SUB), :]
            )
            return jnp.concatenate([body, halo], axis=0)

        total = length + SUB
        shift_down = lambda x: pltpu.roll(x, 1, 0)
        shift_up = lambda x: pltpu.roll(x, total - 1, 0)
        for half, (s, r) in enumerate(((0, 2), (1, 3))):
            smooth, rough = window(s), window(r)
            if half == 0:
                smooth = smooth * big
            else:
                rough = rough * small
            smooth, rough = lifted(smooth, rough, shift_down, shift_up)
            joined[half, c, pl.ds(0, length, stride=2), :] = smooth[:length]
            joined[half, c, pl.ds(1, length, stride=2), :] = rough[:length]

    def horizontal(tiles, load, store, last):
        smooth = [load(0, c) for c in range(tiles + 1)]
        rough = [load(1, c) for c in range(tiles + 1)]

        def before(x):
            turned = [pltpu.roll(t, 1, 1) for t in x]
            return [jnp.where(lane == 0, turned[c - 1], turned[c]) for c in range(tiles + 1)]

        def after(x):
            turned = [pltpu.roll(t, LANES - 1, 1) for t in x]
            return [
                jnp.where(lane == LANES - 1, turned[(c + 1) % (tiles + 1)], turned[c])
                for c in range(tiles + 1)
            ]

        def step(x, factor, y, z):
            return [a - factor * (b + c) for a, b, c in zip(x, y, z)]

        smooth = step(smooth, lift_delta, rough, before(rough))
        rough = step(rough, lift_gamma, smooth, after(smooth))
        smooth = step(smooth, lift_beta, rough, before(rough))
        rough = step(rough, lift_alpha, smooth, after(smooth))
        for c in range(tiles if last else tiles + 1):
            first = jnp.where(low, smooth[c], rough[c])
            second = jnp.where(low, rough[c], smooth[c])
            first = jnp.take_along_axis(first, pick_low, axis=1, mode="promise_in_bounds")
            second = jnp.take_along_axis(second, pick_high, axis=1, mode="promise_in_bounds")
            left = jnp.where(even, first, second)
            right = jnp.where(even, second, first)
            if c < tiles:
                store(2 * c, left)
                store(2 * c + 1, right)
            else:
                store(2 * c, jnp.where(low, left, right))

    stores = []
    for level, (height, width) in enumerate(sizes):
        tiles = width // LANES
        last = level == count - 1
        rows = min(chunk_rows, height)
        chunks = height // rows
        ref = bands[level]
        target = finished if last else bands[level + 1].at[0]
        for copy in loads[level]:
            copy.wait()

        def one_chunk(i, carry):
            start = pl.multiple_of(i * rows, SUB)
            before = pl.multiple_of(jnp.where(i == 0, height, start - SUB), SUB)
            after = pl.multiple_of(start + rows, SUB)

            def one_column(c, carry):
                vertical(ref, c, start, rows, before, after)
                return carry

            lax.fori_loop(0, tiles + 1, one_column, 0)

            def one_row(t, carry):
                where = pl.ds(pl.multiple_of(t * SUB, SUB), SUB)
                into = pl.ds(pl.multiple_of(2 * start + t * SUB, SUB), SUB)

                def store(c, value):
                    target[c, into, :] = value

                horizontal(tiles, lambda half, c: joined[half, c, where, :], store, last)
                return carry

            lax.fori_loop(0, 2 * rows // SUB, one_row, 0)
            return carry

        if last:
            for i in range(chunks):
                one_chunk(i, 0)
                span = pl.ds(2 * i * rows, 2 * rows)
                for c in range(2 * tiles):
                    copy = pltpu.make_async_copy(
                        finished.at[c, span, :],
                        out.at[span, pl.ds(c * LANES, LANES)],
                        store_sem.at[len(stores)],
                    )
                    copy.start()
                    stores.append(copy)
        else:
            lax.fori_loop(0, chunks, one_chunk, 0)

            def edge_column(c, carry):
                vertical(ref, c, height, SUB, height - SUB, 0)
                return carry

            lax.fori_loop(0, tiles + 1, edge_column, 0)

            def load(half, c):
                return jnp.where(
                    sub < 4, joined[half, c, pl.ds(0, SUB), :], joined[half, c, pl.ds(SUB, SUB), :]
                )

            def store(c, value):
                target[c, pl.ds(2 * height, SUB), :] = value

            horizontal(tiles, load, store, False)
    for copy in stores:
        copy.wait()


def per_device(mesh_shape, coarse, *details):
    arrays = (coarse[None],) + details
    levels = [a.shape for a in arrays]
    sizes = [d.shape[1:] for d in details]
    f32 = jnp.float32
    shape = lambda *dims: jax.ShapeDtypeStruct(dims, f32)
    packed_rows = sum(b * (h // groups_of(h)) for b, h, w in levels)
    strips = [shape(b, SUB, w) for b, h, w in levels]
    anywhere = pl.BlockSpec(memory_space=pl.ANY)
    in_vmem = pl.BlockSpec(memory_space=pltpu.VMEM)
    n = len(levels)
    halo_shapes = strips + strips + [shape(packed_rows, LANES)] * 2 + [shape(SUB, LANES)] * 4
    n_sends = 2 * n + 6
    halos = pl.pallas_call(
        functools.partial(exchange, mesh_shape, levels),
        out_shape=halo_shapes,
        in_specs=[anywhere] * n,
        out_specs=[anywhere] * len(halo_shapes),
        scratch_shapes=[
            pltpu.VMEM((packed_rows, LANES), f32),
            pltpu.VMEM((SUB, LANES), f32),
            pltpu.VMEM((SUB, LANES), f32),
        ]
        + [pltpu.VMEM((b, h, LANES), f32) for b, h, w in levels] * 2
        + [
            pltpu.SemaphoreType.DMA((2 * n,)),
            pltpu.SemaphoreType.DMA((n_sends,)),
            pltpu.SemaphoreType.DMA((n_sends,)),
        ],
        compiler_params=pltpu.CompilerParams(collective_id=0, has_side_effects=True),
        name="exchange",
    )(*arrays)

    chunk_rows = 64
    height, width = sizes[-1]
    n_loads = sum(w // LANES for h, w in sizes) + sizes[0][1] // LANES
    n_stores = (height // min(chunk_rows, height)) * (2 * width // LANES)
    return pl.pallas_call(
        functools.partial(synthesis, sizes, chunk_rows),
        out_shape=shape(2 * height, 2 * width),
        in_specs=[anywhere] * n + [in_vmem] * len(halo_shapes),
        out_specs=anywhere,
        scratch_shapes=[
            pltpu.VMEM((4, w // LANES + 1, h + SUB, LANES), f32) for h, w in sizes
        ]
        + [
            pltpu.VMEM((2, width // LANES + 1, 2 * min(chunk_rows, height), LANES), f32),
            pltpu.VMEM((2 * width // LANES, 2 * height, LANES), f32),
            pltpu.SemaphoreType.DMA((n_loads,)),
            pltpu.SemaphoreType.DMA((n_stores,)),
        ],
        compiler_params=pltpu.CompilerParams(vmem_limit_bytes=56 * 1024 * 1024),
        name="synthesis",
    )(*arrays, *halos)


def solution(mesh):
    mesh_shape = (mesh.shape["rows"], mesh.shape["cols"])
    return jax.shard_map(
        functools.partial(per_device, mesh_shape),
        mesh=mesh,
        in_specs=(
            P("rows", "cols"),
            P(None, "rows", "cols"),
            P(None, "rows", "cols"),
            P(None, "rows", "cols"),
            P(None, "rows", "cols"),
        ),
        out_specs=P("rows", "cols"),
        check_vma=False,
    )
```

```python
import functools
import math

import jax
import jax.numpy as jnp
from jax import lax
from jax.experimental import pallas as pl
from jax.experimental.pallas import tpu as pltpu
from jax.sharding import PartitionSpec as P

lift_alpha = -1.586134342059924
lift_beta = -0.052980118572961
lift_gamma = 0.882911075530934
lift_delta = 0.443506852043971
lift_scale = 1.149604398860241

MESH = pl.DeviceIdType.MESH
LANES = 128
SUB = 8
UNROLL = 4


def groups_of(height):
    return min(16, height // SUB)


def lanes_of(shape):
    return lax.broadcasted_iota(jnp.int32, shape, len(shape) - 1)


def rows_of(shape):
    return lax.broadcasted_iota(jnp.int32, shape, len(shape) - 2)


def exchange(mesh_shape, levels, *refs):
    count = len(levels)
    inputs, refs = refs[:count], refs[count:]
    below, above, refs = refs[:count], refs[count : 2 * count], refs[2 * count :]
    from_right, from_left, down_right, down_left, up_right, up_left, *refs = refs
    packed, top, bottom, *refs = refs
    firsts, lasts, refs = refs[:count], refs[count : 2 * count], refs[2 * count :]
    local_sem, send_sem, recv_sem = refs

    n_rows, n_cols = mesh_shape
    row, col = lax.axis_index("rows"), lax.axis_index("cols")
    row_next, row_prev = lax.rem(row + 1, n_rows), lax.rem(row + n_rows - 1, n_rows)
    col_next, col_prev = lax.rem(col + 1, n_cols), lax.rem(col + n_cols - 1, n_cols)

    barrier = pltpu.get_barrier_semaphore()
    neighbours = [
        (r, c)
        for r in (row_prev, row, row_next)
        for c in (col_prev, col, col_next)
        if not (r is row and c is col)
    ]
    for place in neighbours:
        pl.semaphore_signal(barrier, inc=1, device_id=place, device_id_type=MESH)

    loads = []
    for i, (bands, height, width) in enumerate(levels):
        for j, (slab, start) in enumerate(((firsts[i], 0), (lasts[i], width - LANES))):
            copy = pltpu.make_async_copy(
                inputs[i].at[:, :, pl.ds(start, LANES)], slab, local_sem.at[2 * i + j]
            )
            copy.start()
            loads.append(copy)

    pl.semaphore_wait(barrier, len(neighbours))

    sends = []

    def send(src, dst, place):
        k = len(sends)
        copy = pltpu.make_async_remote_copy(
            src_ref=src,
            dst_ref=dst,
            send_sem=send_sem.at[k],
            recv_sem=recv_sem.at[k],
            device_id=place,
            device_id_type=MESH,
        )
        copy.start()
        sends.append(copy)

    for i in reversed(range(count)):
        height = levels[i][1]
        send(inputs[i].at[:, pl.ds(0, SUB), :], below[i], (row_prev, col))
        send(inputs[i].at[:, pl.ds(height - SUB, SUB), :], above[i], (row_next, col))

    for copy in loads:
        copy.wait()

    tops = bottoms = None
    offset = place = 0
    for i, (bands, height, width) in enumerate(levels):
        groups = groups_of(height)
        part = height // groups
        lane = lanes_of((part, LANES))
        slot = lax.rem(lane + 4, LANES) // 8
        lane8 = lanes_of((SUB, LANES))
        slot8 = lax.rem(lane8 + 4, LANES) // 8
        for b in range(bands):
            total = None
            for g in range(groups):
                rows = pl.ds(g * part, part)
                edge = jnp.where(lane < 64, firsts[i][b, rows, :], lasts[i][b, rows, :])
                if g:
                    edge = pltpu.roll(edge, 8 * g, 1)
                total = edge if total is None else jnp.where(slot == g, edge, total)
            packed[pl.ds(offset, part), :] = total
            offset += part
            for end in range(2):
                rows = pl.ds(0 if end == 0 else height - SUB, SUB)
                edge = jnp.where(lane8 < 64, firsts[i][b, rows, :], lasts[i][b, rows, :])
                if place:
                    edge = pltpu.roll(edge, 8 * place, 1)
                if end == 0:
                    tops = edge if tops is None else jnp.where(slot8 == place, edge, tops)
                else:
                    bottoms = edge if bottoms is None else jnp.where(slot8 == place, edge, bottoms)
            place += 1
    top[...] = tops
    bottom[...] = bottoms

    send(packed, from_right, (row, col_prev))
    send(packed, from_left, (row, col_next))
    send(top, down_right, (row_prev, col_prev))
    send(top, down_left, (row_prev, col_next))
    send(bottom, up_right, (row_next, col_prev))
    send(bottom, up_left, (row_next, col_next))
    for copy in sends:
        copy.wait()


def lifted(smooth, rough, before, after):
    smooth = smooth - lift_delta * (rough + before(rough))
    rough = rough - lift_gamma * (smooth + after(smooth))
    smooth = smooth - lift_beta * (rough + before(rough))
    rough = rough - lift_alpha * (smooth + after(smooth))
    return smooth, rough


def synthesis(sizes, chunk_rows, *refs):
    count = len(sizes)
    arrays = count + 1
    inputs, refs = refs[:arrays], refs[arrays:]
    below, above, refs = refs[:arrays], refs[arrays : 2 * arrays], refs[2 * arrays :]
    from_right, from_left, down_right, down_left, up_right, up_left, out, *refs = refs
    bands, joined, refs = refs[:count], refs[count], refs[count + 1 :]
    finished, load_sem, store_sem = refs

    loads = []
    k = 0
    for level, (height, width) in enumerate(sizes):
        mine = []
        for c in range(width // LANES):
            columns = pl.ds(c * LANES, LANES)
            if level == 0:
                copy = pltpu.make_async_copy(
                    inputs[0].at[:, :, columns],
                    bands[0].at[pl.ds(0, 1), c, pl.ds(0, height), :],
                    load_sem.at[k],
                )
                copy.start()
                mine.append(copy)
                k += 1
            copy = pltpu.make_async_copy(
                inputs[level + 1].at[:, :, columns],
                bands[level].at[pl.ds(1, 3), c, pl.ds(0, height), :],
                load_sem.at[k],
            )
            copy.start()
            mine.append(copy)
            k += 1
        loads.append(mine)

    lane = lanes_of((SUB, LANES))
    sub = rows_of((SUB, LANES))
    even = lax.rem(lane, 2) == 0
    low = lane < 64
    pick_low = lane // 2 + jnp.where(even, 0, 64)
    pick_high = lane // 2 + jnp.where(even, 64, 0)
    right_side = lax.rem(lane, 8) < 4

    corner = jnp.where(
        sub < 4,
        jnp.where(right_side, down_right[...], down_left[...]),
        jnp.where(right_side, up_right[...], up_left[...]),
    )
    offset = place = 0
    for i in range(arrays):
        level = max(i - 1, 0)
        height, width = sizes[level]
        groups = groups_of(height)
        part = height // groups
        tiles = width // LANES
        wide = lax.rem(lanes_of((part, LANES)), 8) < 4
        for b in range(1 if i == 0 else 3):
            ref = bands[level].at[b if i == 0 else b + 1]
            rows = pl.ds(offset, part)
            edge = jnp.where(wide, from_right[rows, :], from_left[rows, :])
            for g in range(groups):
                ref[tiles, pl.ds(g * part, part), :] = (
                    pltpu.roll(edge, LANES - 8 * g, 1) if g else edge
                )
            offset += part
            for c in range(tiles):
                columns = pl.ds(c * LANES, LANES)
                ref[c, pl.ds(height, SUB), :] = jnp.where(
                    sub < 4, below[i][b, :, columns], above[i][b, :, columns]
                )
            ref[tiles, pl.ds(height, SUB), :] = (
                pltpu.roll(corner, LANES - 8 * place, 1) if place else corner
            )
            place += 1

    big, small = lift_scale * lift_scale, 1.0 / (lift_scale * lift_scale)

    def vertical(ref, c, start, length, before, after):
        def window(b):
            body = ref[b, c, pl.ds(start, length), :]
            halo = jnp.where(
                sub < 4, ref[b, c, pl.ds(after, SUB), :], ref[b, c, pl.ds(before, SUB), :]
            )
            return jnp.concatenate([body, halo], axis=0)

        total = length + SUB
        shift_down = lambda x: pltpu.roll(x, 1, 0)
        shift_up = lambda x: pltpu.roll(x, total - 1, 0)
        for half, (s, r) in enumerate(((0, 2), (1, 3))):
            smooth, rough = window(s), window(r)
            if half == 0:
                smooth = smooth * big
            else:
                rough = rough * small
            smooth, rough = lifted(smooth, rough, shift_down, shift_up)
            joined[half, c, pl.ds(0, length, stride=2), :] = smooth[:length]
            joined[half, c, pl.ds(1, length, stride=2), :] = rough[:length]

    def horizontal(tiles, load, store, last):
        smooth = [load(0, c) for c in range(tiles + 1)]
        rough = [load(1, c) for c in range(tiles + 1)]

        def before(x):
            turned = [pltpu.roll(t, 1, 1) for t in x]
            return [jnp.where(lane == 0, turned[c - 1], turned[c]) for c in range(tiles + 1)]

        def after(x):
            turned = [pltpu.roll(t, LANES - 1, 1) for t in x]
            return [
                jnp.where(lane == LANES - 1, turned[(c + 1) % (tiles + 1)], turned[c])
                for c in range(tiles + 1)
            ]

        def step(x, factor, y, z):
            return [a - factor * (b + c) for a, b, c in zip(x, y, z)]

        smooth = step(smooth, lift_delta, rough, before(rough))
        rough = step(rough, lift_gamma, smooth, after(smooth))
        smooth = step(smooth, lift_beta, rough, before(rough))
        rough = step(rough, lift_alpha, smooth, after(smooth))
        for c in range(tiles if last else tiles + 1):
            first = jnp.where(low, smooth[c], rough[c])
            second = jnp.where(low, rough[c], smooth[c])
            first = jnp.take_along_axis(first, pick_low, axis=1, mode="promise_in_bounds")
            second = jnp.take_along_axis(second, pick_high, axis=1, mode="promise_in_bounds")
            left = jnp.where(even, first, second)
            right = jnp.where(even, second, first)
            if c < tiles:
                store(2 * c, left)
                store(2 * c + 1, right)
            else:
                store(2 * c, jnp.where(low, left, right))

    stores = []
    for level, (height, width) in enumerate(sizes):
        tiles = width // LANES
        last = level == count - 1
        rows = min(chunk_rows, height)
        chunks = height // rows
        unroll = math.gcd(max(UNROLL, 16 // tiles), 2 * rows // SUB)
        ref = bands[level]
        target = finished if last else bands[level + 1].at[0]
        for copy in loads[level]:
            copy.wait()

        def one_chunk(i, carry):
            start = pl.multiple_of(i * rows, SUB)
            before = pl.multiple_of(jnp.where(i == 0, height, start - SUB), SUB)
            after = pl.multiple_of(start + rows, SUB)

            def one_column(c, carry):
                vertical(ref, c, start, rows, before, after)
                return carry

            lax.fori_loop(0, tiles + 1, one_column, 0)

            def one_row(t, carry):
                for u in range(unroll):
                    first = (t * unroll + u) * SUB
                    where = pl.ds(pl.multiple_of(first, SUB), SUB)
                    into = pl.ds(pl.multiple_of(2 * start + first, SUB), SUB)

                    def store(c, value, into=into):
                        target[c, into, :] = value

                    def load(half, c, where=where):
                        return joined[half, c, where, :]

                    horizontal(tiles, load, store, last)
                return carry

            lax.fori_loop(0, 2 * rows // (SUB * unroll), one_row, 0)
            return carry

        if last:
            for i in range(chunks):
                one_chunk(i, 0)
                span = pl.ds(2 * i * rows, 2 * rows)
                for c in range(2 * tiles):
                    copy = pltpu.make_async_copy(
                        finished.at[c, span, :],
                        out.at[span, pl.ds(c * LANES, LANES)],
                        store_sem.at[len(stores)],
                    )
                    copy.start()
                    stores.append(copy)
        else:
            lax.fori_loop(0, chunks, one_chunk, 0)

            def edge_column(c, carry):
                vertical(ref, c, height, SUB, height - SUB, 0)
                return carry

            lax.fori_loop(0, tiles + 1, edge_column, 0)

            def load(half, c):
                return jnp.where(
                    sub < 4, joined[half, c, pl.ds(0, SUB), :], joined[half, c, pl.ds(SUB, SUB), :]
                )

            def store(c, value):
                target[c, pl.ds(2 * height, SUB), :] = value

            horizontal(tiles, load, store, False)
    for copy in stores:
        copy.wait()


def per_device(mesh_shape, coarse, *details):
    arrays = (coarse[None],) + details
    levels = [a.shape for a in arrays]
    sizes = [d.shape[1:] for d in details]
    f32 = jnp.float32
    shape = lambda *dims: jax.ShapeDtypeStruct(dims, f32)
    packed_rows = sum(b * (h // groups_of(h)) for b, h, w in levels)
    strips = [shape(b, SUB, w) for b, h, w in levels]
    anywhere = pl.BlockSpec(memory_space=pl.ANY)
    in_vmem = pl.BlockSpec(memory_space=pltpu.VMEM)
    n = len(levels)
    halo_shapes = strips + strips + [shape(packed_rows, LANES)] * 2 + [shape(SUB, LANES)] * 4
    n_sends = 2 * n + 6
    halos = pl.pallas_call(
        functools.partial(exchange, mesh_shape, levels),
        out_shape=halo_shapes,
        in_specs=[anywhere] * n,
        out_specs=[anywhere] * len(halo_shapes),
        scratch_shapes=[
            pltpu.VMEM((packed_rows, LANES), f32),
            pltpu.VMEM((SUB, LANES), f32),
            pltpu.VMEM((SUB, LANES), f32),
        ]
        + [pltpu.VMEM((b, h, LANES), f32) for b, h, w in levels] * 2
        + [
            pltpu.SemaphoreType.DMA((2 * n,)),
            pltpu.SemaphoreType.DMA((n_sends,)),
            pltpu.SemaphoreType.DMA((n_sends,)),
        ],
        compiler_params=pltpu.CompilerParams(collective_id=0, has_side_effects=True),
        name="exchange",
    )(*arrays)

    chunk_rows = 64
    height, width = sizes[-1]
    n_loads = sum(w // LANES for h, w in sizes) + sizes[0][1] // LANES
    n_stores = (height // min(chunk_rows, height)) * (2 * width // LANES)
    return pl.pallas_call(
        functools.partial(synthesis, sizes, chunk_rows),
        out_shape=shape(2 * height, 2 * width),
        in_specs=[anywhere] * n + [in_vmem] * len(halo_shapes),
        out_specs=anywhere,
        scratch_shapes=[
            pltpu.VMEM((4, w // LANES + 1, h + SUB, LANES), f32) for h, w in sizes
        ]
        + [
            pltpu.VMEM((2, width // LANES + 1, 2 * min(chunk_rows, height), LANES), f32),
            pltpu.VMEM((2 * width // LANES, 2 * height, LANES), f32),
            pltpu.SemaphoreType.DMA((n_loads,)),
            pltpu.SemaphoreType.DMA((n_stores,)),
        ],
        compiler_params=pltpu.CompilerParams(vmem_limit_bytes=56 * 1024 * 1024),
        name="synthesis",
    )(*arrays, *halos)


def solution(mesh):
    mesh_shape = (mesh.shape["rows"], mesh.shape["cols"])
    return jax.shard_map(
        functools.partial(per_device, mesh_shape),
        mesh=mesh,
        in_specs=(
            P("rows", "cols"),
            P(None, "rows", "cols"),
            P(None, "rows", "cols"),
            P(None, "rows", "cols"),
            P(None, "rows", "cols"),
        ),
        out_specs=P("rows", "cols"),
        check_vma=False,
    )
```

```python
import functools
import math

import jax
import jax.numpy as jnp
from jax import lax
from jax.experimental import pallas as pl
from jax.experimental.pallas import tpu as pltpu
from jax.sharding import PartitionSpec as P

lift_alpha = -1.586134342059924
lift_beta = -0.052980118572961
lift_gamma = 0.882911075530934
lift_delta = 0.443506852043971
lift_scale = 1.149604398860241

MESH = pl.DeviceIdType.MESH
LANES = 128
SUB = 8
UNROLL = 4


def groups_of(height):
    return min(16, height // SUB)


def lanes_of(shape):
    return lax.broadcasted_iota(jnp.int32, shape, len(shape) - 1)


def rows_of(shape):
    return lax.broadcasted_iota(jnp.int32, shape, len(shape) - 2)


def exchange(mesh_shape, levels, *refs):
    count = len(levels)
    inputs, refs = refs[:count], refs[count:]
    below, above, refs = refs[:count], refs[count : 2 * count], refs[2 * count :]
    from_right, from_left, down_right, down_left, up_right, up_left, *refs = refs
    packed, top, bottom, *refs = refs
    firsts, lasts, refs = refs[:count], refs[count : 2 * count], refs[2 * count :]
    local_sem, send_sem, recv_sem = refs

    n_rows, n_cols = mesh_shape
    row, col = lax.axis_index("rows"), lax.axis_index("cols")
    row_next, row_prev = lax.rem(row + 1, n_rows), lax.rem(row + n_rows - 1, n_rows)
    col_next, col_prev = lax.rem(col + 1, n_cols), lax.rem(col + n_cols - 1, n_cols)

    barrier = pltpu.get_barrier_semaphore()
    neighbours = [
        (r, c)
        for r in (row_prev, row, row_next)
        for c in (col_prev, col, col_next)
        if not (r is row and c is col)
    ]
    for place in neighbours:
        pl.semaphore_signal(barrier, inc=1, device_id=place, device_id_type=MESH)

    loads = []
    for i, (bands, height, width) in enumerate(levels):
        for j, (slab, start) in enumerate(((firsts[i], 0), (lasts[i], width - LANES))):
            copy = pltpu.make_async_copy(
                inputs[i].at[:, :, pl.ds(start, LANES)], slab, local_sem.at[2 * i + j]
            )
            copy.start()
            loads.append(copy)

    pl.semaphore_wait(barrier, len(neighbours))

    sends = []

    def send(src, dst, place):
        k = len(sends)
        copy = pltpu.make_async_remote_copy(
            src_ref=src,
            dst_ref=dst,
            send_sem=send_sem.at[k],
            recv_sem=recv_sem.at[k],
            device_id=place,
            device_id_type=MESH,
        )
        copy.start()
        sends.append(copy)

    for i in reversed(range(count)):
        height = levels[i][1]
        send(inputs[i].at[:, pl.ds(0, SUB), :], below[i], (row_prev, col))
        send(inputs[i].at[:, pl.ds(height - SUB, SUB), :], above[i], (row_next, col))

    for copy in loads:
        copy.wait()

    tops = bottoms = None
    offset = place = 0
    for i, (bands, height, width) in enumerate(levels):
        groups = groups_of(height)
        part = height // groups
        lane = lanes_of((part, LANES))
        slot = lax.rem(lane + 4, LANES) // 8
        lane8 = lanes_of((SUB, LANES))
        slot8 = lax.rem(lane8 + 4, LANES) // 8
        for b in range(bands):
            total = None
            for g in range(groups):
                rows = pl.ds(g * part, part)
                edge = jnp.where(lane < 64, firsts[i][b, rows, :], lasts[i][b, rows, :])
                if g:
                    edge = pltpu.roll(edge, 8 * g, 1)
                total = edge if total is None else jnp.where(slot == g, edge, total)
            packed[pl.ds(offset, part), :] = total
            offset += part
            for end in range(2):
                rows = pl.ds(0 if end == 0 else height - SUB, SUB)
                edge = jnp.where(lane8 < 64, firsts[i][b, rows, :], lasts[i][b, rows, :])
                if place:
                    edge = pltpu.roll(edge, 8 * place, 1)
                if end == 0:
                    tops = edge if tops is None else jnp.where(slot8 == place, edge, tops)
                else:
                    bottoms = edge if bottoms is None else jnp.where(slot8 == place, edge, bottoms)
            place += 1
    top[...] = tops
    bottom[...] = bottoms

    send(packed, from_right, (row, col_prev))
    send(packed, from_left, (row, col_next))
    send(top, down_right, (row_prev, col_prev))
    send(top, down_left, (row_prev, col_next))
    send(bottom, up_right, (row_next, col_prev))
    send(bottom, up_left, (row_next, col_next))
    for copy in sends:
        copy.wait()


def lifted(smooth, rough, before, after):
    smooth = smooth - lift_delta * (rough + before(rough))
    rough = rough - lift_gamma * (smooth + after(smooth))
    smooth = smooth - lift_beta * (rough + before(rough))
    rough = rough - lift_alpha * (smooth + after(smooth))
    return smooth, rough


def synthesis(sizes, chunk_rows, piece_rows, *refs):
    count = len(sizes)
    arrays = count + 1
    inputs, refs = refs[:arrays], refs[arrays:]
    below, above, refs = refs[:arrays], refs[arrays : 2 * arrays], refs[2 * arrays :]
    from_right, from_left, down_right, down_left, up_right, up_left, out, *refs = refs
    bands, joined, refs = refs[:count], refs[count], refs[count + 1 :]
    finished, load_sem, store_sem, *stages = refs

    loads = []
    k = 0
    for level, (height, width) in enumerate(sizes):
        mine = []
        for c in range(width // LANES):
            columns = pl.ds(c * LANES, LANES)
            if level == 0:
                copy = pltpu.make_async_copy(
                    inputs[0].at[:, :, columns],
                    bands[0].at[pl.ds(0, 1), c, pl.ds(0, height), :],
                    load_sem.at[k],
                )
                copy.start()
                mine.append(copy)
                k += 1
            copy = pltpu.make_async_copy(
                inputs[level + 1].at[:, :, columns],
                bands[level].at[pl.ds(1, 3), c, pl.ds(0, height), :],
                load_sem.at[k],
            )
            copy.start()
            mine.append(copy)
            k += 1
        loads.append(mine)

    lane = lanes_of((SUB, LANES))
    sub = rows_of((SUB, LANES))
    even = lax.rem(lane, 2) == 0
    low = lane < 64
    pick_low = lane // 2 + jnp.where(even, 0, 64)
    pick_high = lane // 2 + jnp.where(even, 64, 0)
    right_side = lax.rem(lane, 8) < 4

    corner = jnp.where(
        sub < 4,
        jnp.where(right_side, down_right[...], down_left[...]),
        jnp.where(right_side, up_right[...], up_left[...]),
    )
    offset = place = 0
    for i in range(arrays):
        level = max(i - 1, 0)
        height, width = sizes[level]
        groups = groups_of(height)
        part = height // groups
        tiles = width // LANES
        wide = lax.rem(lanes_of((part, LANES)), 8) < 4
        for b in range(1 if i == 0 else 3):
            ref = bands[level].at[b if i == 0 else b + 1]
            rows = pl.ds(offset, part)
            edge = jnp.where(wide, from_right[rows, :], from_left[rows, :])
            for g in range(groups):
                ref[tiles, pl.ds(g * part, part), :] = (
                    pltpu.roll(edge, LANES - 8 * g, 1) if g else edge
                )
            offset += part
            for c in range(tiles):
                columns = pl.ds(c * LANES, LANES)
                ref[c, pl.ds(height, SUB), :] = jnp.where(
                    sub < 4, below[i][b, :, columns], above[i][b, :, columns]
                )
            ref[tiles, pl.ds(height, SUB), :] = (
                pltpu.roll(corner, LANES - 8 * place, 1) if place else corner
            )
            place += 1

    big, small = lift_scale * lift_scale, 1.0 / (lift_scale * lift_scale)

    def vertical(ref, c, start, length, before, after, into):
        def window(b):
            body = ref[b, c, pl.ds(start, length), :]
            halo = jnp.where(
                sub < 4, ref[b, c, pl.ds(after, SUB), :], ref[b, c, pl.ds(before, SUB), :]
            )
            return jnp.concatenate([body, halo], axis=0)

        total = length + SUB
        shift_down = lambda x: pltpu.roll(x, 1, 0)
        shift_up = lambda x: pltpu.roll(x, total - 1, 0)
        for half, (s, r) in enumerate(((0, 2), (1, 3))):
            smooth, rough = window(s), window(r)
            if half == 0:
                smooth = smooth * big
            else:
                rough = rough * small
            smooth, rough = lifted(smooth, rough, shift_down, shift_up)
            joined[half, c, pl.ds(into, length, stride=2), :] = smooth[:length]
            joined[half, c, pl.ds(into + 1, length, stride=2), :] = rough[:length]

    def rolled_before(x, n):
        turned = [pltpu.roll(t, 1, 1) for t in x]
        return [jnp.where(lane == 0, turned[c - 1], turned[c]) for c in range(n)]

    def rolled_after(x, n):
        turned = [pltpu.roll(t, LANES - 1, 1) for t in x]
        return [jnp.where(lane == LANES - 1, turned[(c + 1) % n], turned[c]) for c in range(n)]

    def step(x, factor, y, z):
        return [a - factor * (b + c) for a, b, c in zip(x, y, z)]

    def interleave(smooth, rough, tiles, store, last):
        for c in range(tiles if last else tiles + 1):
            first = jnp.where(low, smooth[c], rough[c])
            second = jnp.where(low, rough[c], smooth[c])
            first = jnp.take_along_axis(first, pick_low, axis=1, mode="promise_in_bounds")
            second = jnp.take_along_axis(second, pick_high, axis=1, mode="promise_in_bounds")
            left = jnp.where(even, first, second)
            right = jnp.where(even, second, first)
            if c < tiles:
                store(2 * c, left)
                store(2 * c + 1, right)
            else:
                store(2 * c, jnp.where(low, left, right))

    def horizontal(tiles, load, store, last):
        n = tiles + 1
        smooth = [load(0, c) for c in range(n)]
        rough = [load(1, c) for c in range(n)]
        smooth = step(smooth, lift_delta, rough, rolled_before(rough, n))
        rough = step(rough, lift_gamma, smooth, rolled_after(smooth, n))
        smooth = step(smooth, lift_beta, rough, rolled_before(rough, n))
        rough = step(rough, lift_alpha, smooth, rolled_after(smooth, n))
        interleave(smooth, rough, tiles, store, last)

    def pipelined(tiles, total, unroll, target, last, after_step):
        n = tiles + 1
        s1, r1, s2, r2 = stages
        groups = total // (SUB * unroll)

        def body(t, carry):
            def rows_at(group, u):
                first = jnp.clip(group, 0, groups - 1) * (SUB * unroll) + u * SUB
                return pl.ds(pl.multiple_of(first, SUB), SUB)

            def get(buffer, group, u):
                slot = lax.rem(group + 8, 2)
                return [buffer[slot, u, c] for c in range(n)]

            def put(buffer, group, u, value):
                slot = lax.rem(group + 8, 2)
                for c in range(n):
                    buffer[slot, u, c] = value[c]

            for u in range(unroll):
                into = rows_at(t - 4, u)

                def store(c, value, into=into):
                    target[c, into, :] = value

                interleave(get(s2, t - 4, u), get(r2, t - 4, u), tiles, store, last)
            for u in range(unroll):
                smooth = get(s2, t - 3, u)
                put(r2, t - 3, u, step(get(r1, t - 3, u), lift_alpha, smooth, rolled_after(smooth, n)))
            for u in range(unroll):
                rough = get(r1, t - 2, u)
                put(s2, t - 2, u, step(get(s1, t - 2, u), lift_beta, rough, rolled_before(rough, n)))
            for u in range(unroll):
                smooth = get(s1, t - 1, u)
                rough = [joined[1, c, rows_at(t - 1, u), :] for c in range(n)]
                put(r1, t - 1, u, step(rough, lift_gamma, smooth, rolled_after(smooth, n)))
            for u in range(unroll):
                smooth = [joined[0, c, rows_at(t, u), :] for c in range(n)]
                rough = [joined[1, c, rows_at(t, u), :] for c in range(n)]
                put(s1, t, u, step(smooth, lift_delta, rough, rolled_before(rough, n)))
            after_step(t - 4, groups)
            return carry

        lax.fori_loop(0, groups + 4, body, 0)

    for level, (height, width) in enumerate(sizes):
        tiles = width // LANES
        last = level == count - 1
        rows = min(chunk_rows, height)
        chunks = height // rows
        unroll = math.gcd(max(UNROLL, 16 // tiles), 2 * rows // SUB)
        ref = bands[level]
        target = finished if last else bands[level + 1].at[0]
        for copy in loads[level]:
            copy.wait()

        def one_chunk(i, carry):
            start = pl.multiple_of(i * rows, SUB)
            before = pl.multiple_of(jnp.where(i == 0, height, start - SUB), SUB)
            after = pl.multiple_of(start + rows, SUB)
            into = pl.multiple_of(2 * start, SUB)

            def one_column(c, carry):
                vertical(ref, c, start, rows, before, after, into)
                return carry

            lax.fori_loop(0, tiles + 1, one_column, 0)
            return carry

        lax.fori_loop(0, chunks, one_chunk, 0)

        def store_copy(piece, c):
            span = pl.ds(pl.multiple_of(piece * piece_rows, SUB), piece_rows)
            return pltpu.make_async_copy(
                finished.at[c, span, :],
                out.at[span, pl.ds(c * LANES, LANES)],
                store_sem.at[piece, c],
            )

        if tiles >= 4:
            unroll = UNROLL if last else 2 * UNROLL

            def after_step(group, groups):
                if not last:
                    return
                every = piece_rows // (SUB * unroll)

                @pl.when((group >= 0) & (lax.rem(group + every, every) == every - 1))
                def _():
                    for c in range(2 * tiles):
                        store_copy(group // every, c).start()

            pipelined(tiles, 2 * height, unroll, target, last, after_step)
        else:
            unroll = math.gcd(16, 2 * height // SUB)

            def one_row(t, carry):
                for u in range(unroll):
                    where = pl.ds(pl.multiple_of((t * unroll + u) * SUB, SUB), SUB)

                    def store(c, value, where=where):
                        target[c, where, :] = value

                    def load(half, c, where=where):
                        return joined[half, c, where, :]

                    horizontal(tiles, load, store, last)
                return carry

            lax.fori_loop(0, 2 * height // (SUB * unroll), one_row, 0)

        if not last:

            def edge_column(c, carry):
                vertical(ref, c, height, SUB, height - SUB, 0, 0)
                return carry

            lax.fori_loop(0, tiles + 1, edge_column, 0)

            def load(half, c):
                return jnp.where(
                    sub < 4, joined[half, c, pl.ds(0, SUB), :], joined[half, c, pl.ds(SUB, SUB), :]
                )

            def store(c, value):
                target[c, pl.ds(2 * height, SUB), :] = value

            horizontal(tiles, load, store, False)
        else:
            for piece in range(2 * height // piece_rows):
                for c in range(2 * tiles):
                    store_copy(piece, c).wait()


def per_device(mesh_shape, coarse, *details):
    arrays = (coarse[None],) + details
    levels = [a.shape for a in arrays]
    sizes = [d.shape[1:] for d in details]
    f32 = jnp.float32
    shape = lambda *dims: jax.ShapeDtypeStruct(dims, f32)
    packed_rows = sum(b * (h // groups_of(h)) for b, h, w in levels)
    strips = [shape(b, SUB, w) for b, h, w in levels]
    anywhere = pl.BlockSpec(memory_space=pl.ANY)
    in_vmem = pl.BlockSpec(memory_space=pltpu.VMEM)
    n = len(levels)
    halo_shapes = strips + strips + [shape(packed_rows, LANES)] * 2 + [shape(SUB, LANES)] * 4
    n_sends = 2 * n + 6
    halos = pl.pallas_call(
        functools.partial(exchange, mesh_shape, levels),
        out_shape=halo_shapes,
        in_specs=[anywhere] * n,
        out_specs=[anywhere] * len(halo_shapes),
        scratch_shapes=[
            pltpu.VMEM((packed_rows, LANES), f32),
            pltpu.VMEM((SUB, LANES), f32),
            pltpu.VMEM((SUB, LANES), f32),
        ]
        + [pltpu.VMEM((b, h, LANES), f32) for b, h, w in levels] * 2
        + [
            pltpu.SemaphoreType.DMA((2 * n,)),
            pltpu.SemaphoreType.DMA((n_sends,)),
            pltpu.SemaphoreType.DMA((n_sends,)),
        ],
        compiler_params=pltpu.CompilerParams(collective_id=0, has_side_effects=True),
        name="exchange",
    )(*arrays)

    chunk_rows = 64
    height, width = sizes[-1]
    n_loads = sum(w // LANES for h, w in sizes) + sizes[0][1] // LANES
    piece_rows = math.gcd(128, 2 * height)
    return pl.pallas_call(
        functools.partial(synthesis, sizes, chunk_rows, piece_rows),
        out_shape=shape(2 * height, 2 * width),
        in_specs=[anywhere] * n + [in_vmem] * len(halo_shapes),
        out_specs=anywhere,
        scratch_shapes=[
            pltpu.VMEM((4, w // LANES + 1, h + SUB, LANES), f32) for h, w in sizes
        ]
        + [
            pltpu.VMEM((2, width // LANES + 1, 2 * height, LANES), f32),
            pltpu.VMEM((2 * width // LANES, 2 * height, LANES), f32),
            pltpu.SemaphoreType.DMA((n_loads,)),
            pltpu.SemaphoreType.DMA((2 * height // piece_rows, 2 * width // LANES)),
        ]
        + [pltpu.VMEM((2, 2 * UNROLL, width // LANES + 1, SUB, LANES), f32)] * 4,
        compiler_params=pltpu.CompilerParams(vmem_limit_bytes=56 * 1024 * 1024),
        name="synthesis",
    )(*arrays, *halos)


def solution(mesh):
    mesh_shape = (mesh.shape["rows"], mesh.shape["cols"])
    return jax.shard_map(
        functools.partial(per_device, mesh_shape),
        mesh=mesh,
        in_specs=(
            P("rows", "cols"),
            P(None, "rows", "cols"),
            P(None, "rows", "cols"),
            P(None, "rows", "cols"),
            P(None, "rows", "cols"),
        ),
        out_specs=P("rows", "cols"),
        check_vma=False,
    )
```
